512 devices in a mesh: group: 16 (over y, x_lo, core), tile: 32 (over x_hi, z).
Axes of the slice: x: 4 (x_hi: 2, x_lo: 2; x = x_hi * 2 + x_lo), y: 4, z: 16, core: 2. Of those that a mesh axis runs over, the one named last changes fastest.
Arguments:
- checkpoint: float32 [16, 8192, 768], P(None, ('group', 'tile')), may hold values from -6 to 6
- adjoint_in: float32 [16, 8192, 768], P(None, ('group', 'tile')), may hold values from -6 to 6
- courant_x: float32 [16, 8192, 768], P(None, ('group', 'tile')), may hold values from 0.05 to 0.5
- courant_y: float32 [16, 8192, 768], P(None, ('group', 'tile')), may hold values from 0.05 to 0.5
- mixing: float32 [15, 8192, 768], P(None, ('group', 'tile')), may hold values from 0.02 to 0.3
- snd_column: int32 [512, 32, 128], P(('group', 'tile')), may hold values from 0 to 12287
- snd_count: int32 [512, 32], P(('group', 'tile')), may hold values from 32 to 128, as said below
- snd_step: int32 [512, 32, 128], P(('group', 'tile')), may hold values from 0 to 1
- snd_value: float32 [512, 32, 128], P(('group', 'tile')), may hold values from -6 to 6
- snd_weight: float32 [512, 32, 128], P(('group', 'tile')), may hold values from 0.3 to 3
- snd_kernel: float32 [512, 32, 16, 128], P(('group', 'tile')), may hold values from 0 to 0.5
Outputs:
- adjoint_out: float32 [16, 8192, 768], P(None, ('group', 'tile'))
The draws below stay inside these ranges and needn't reach their ends.
Inputs may be any that keep to these rules, and one draw needn't show every extreme that they name: `snd_count`: at most 128; in every draw some destination tile receives 128 soundings from every source device of each group, and every source device fills all slots of some destination tile.
All inputs are finite; a program needn't handle non-finite values.
Results may differ from the reference program's by a relative error of at most 0.0001.
Values sent between devices are 32-bit elements; how exact they have to be, the bound alone decides.
No kernel may reach another device: no remote copies, remote signals or barrier semaphores. Data moves between devices by JAX's collectives and lax.ppermute only.
A program may use at most 64 MiB of HBM per device.

```python
import math
import jax
import jax.numpy as jnp
from jax import lax

LEV = 16
CX = 16
CY = 768
CAP = 128
STEPS = 2
NX = 8192
N_GROUP = 16
N_TILE = 32


def draw_snd_count(key, part):
    key_base, key_crowd, key_chosen, key_forced = jax.random.split(jax.random.fold_in(key, 17), 4)
    device_total = N_GROUP * N_TILE
    drawn = jax.random.randint(key_base, (device_total, N_TILE), CAP // 4, CAP // 2 + 1)
    tiles = jnp.arange(N_TILE, dtype=jnp.int32)
    crowded = jax.random.randint(key_crowd, (N_TILE,), 0, 6) == 0
    chosen = jax.random.randint(key_chosen, (), 0, N_TILE)
    crowded = crowded | (tiles == chosen)
    forced = jax.random.randint(key_forced, (device_total,), 0, N_TILE)
    filled = crowded[None, :] | (tiles[None, :] == forced[:, None])
    return jnp.where(filled, CAP, drawn).astype(jnp.int32)


def touch_ends(result, stream_key, smallest, top_value):
    extent = result.shape
    index_at = [jax.random.randint(jax.random.fold_in(stream_key, axis), (), 0, extent[axis]) for axis in range(len(extent))]
    result = result.at[tuple(index_at)].set(smallest)
    longest = extent.index(max(extent))
    index_at[longest] = (index_at[longest] + 1) % extent[longest]
    return result.at[tuple(index_at)].set(top_value)


def level_of(rng, dims, cuts, low, high):
    def one(axis_at, parts):
        heights = jax.random.uniform(jax.random.fold_in(jax.random.fold_in(rng, 6), axis_at), (parts,), jnp.float32, low / len(cuts), high / len(cuts))
        return jnp.repeat(jnp.exp(heights), dims[axis_at] // parts).reshape((-1,) + (1,) * (len(dims) - axis_at - 1))

    gain = one(*cuts[0])
    for cut in cuts[1:]:
        gain = gain * one(*cut)
    return gain


def centred(key, dims, scale, bound, shards=(), kind=jnp.bfloat16):
    result = scale * jax.random.normal(key, dims, jnp.float32)
    if shards:
        result = result * level_of(key, dims, shards, -0.22, 0.18)
    return jnp.clip(result, -bound, bound).astype(kind)


def setup_inputs(seed: int = 0) -> dict:
    key_list = jax.random.split(jax.random.key(seed), 12)
    return {
        "checkpoint": centred(key_list[0], (LEV, NX, CY), 1.0, 6.0, ((1, 512),), jnp.float32),
        "adjoint_in": centred(key_list[1], (LEV, NX, CY), 1.0, 6.0, ((1, 512),), jnp.float32),
        "courant_x": jnp.clip(jnp.exp(math.log(0.5) - 2.3025851 * jax.random.uniform(key_list[2], (LEV, NX, CY), jnp.float32) ** level_of(key_list[2], (LEV, NX, CY), ((1, 512),), -0.2, 0.2)), 0.05, 0.5),
        "courant_y": jnp.clip(jnp.exp(math.log(0.5) - 2.3025851 * jax.random.uniform(key_list[3], (LEV, NX, CY), jnp.float32) ** level_of(key_list[3], (LEV, NX, CY), ((1, 512),), -0.2, 0.2)), 0.05, 0.5),
        "mixing": jnp.clip(jnp.exp(math.log(0.3) - 2.7080503 * jax.random.uniform(key_list[4], (LEV - 1, NX, CY), jnp.float32) ** level_of(key_list[4], (LEV - 1, NX, CY), ((1, 512),), -0.2, 0.2)), 0.02, 0.3),
        "snd_column": touch_ends(jax.random.randint(key_list[5], (N_GROUP * N_TILE, N_TILE, CAP), 0, CX * CY), jax.random.fold_in(key_list[5], 1), 0, (CX * CY) - 1).astype(jnp.int32),
        "snd_count": draw_snd_count(jax.random.fold_in(key_list[11], 71), 0),
        "snd_step": touch_ends(jax.random.randint(key_list[7], (N_GROUP * N_TILE, N_TILE, CAP), 0, STEPS), jax.random.fold_in(key_list[7], 1), 0, STEPS - 1).astype(jnp.int32),
        "snd_value": centred(key_list[8], (N_GROUP * N_TILE, N_TILE, CAP), 1.0, 6.0, ((0, 512),), jnp.float32),
        "snd_weight": jnp.clip(jnp.exp(math.log(3.0) - 2.3025851 * jax.random.uniform(key_list[9], (N_GROUP * N_TILE, N_TILE, CAP), jnp.float32) ** level_of(key_list[9], (N_GROUP * N_TILE, N_TILE, CAP), ((0, 512),), -0.2, 0.2)), 0.3, 3.0),
        "snd_kernel": jnp.clip(0.5 * jax.random.uniform(key_list[10], (N_GROUP * N_TILE, N_TILE, LEV, CAP), jnp.float32) ** level_of(key_list[10], (N_GROUP * N_TILE, N_TILE, LEV, CAP), ((0, 512),), -0.2, 0.2), 0.0, 0.5),
    }


def pad_periodic(field, width, along):
    total = field.shape[along]
    return jnp.concatenate([lax.slice_in_dim(field, total - width, total, axis=along), field, lax.slice_in_dim(field, 0, width, axis=along)], axis=along)


def sweep_forward(padded, courant_pad, along):
    interior = padded.shape[along] - 4

    def piece_of(first, last):
        return lax.slice_in_dim(padded, first, last, axis=along)

    courant_face = lax.slice_in_dim(courant_pad, 0, interior + 1, axis=along)
    fluxes = courant_face * (2.0 * piece_of(2, interior + 3) + 5.0 * piece_of(1, interior + 2) - piece_of(0, interior + 1)) / 6.0
    return piece_of(2, interior + 2) + lax.slice_in_dim(fluxes, 0, interior, axis=along) - lax.slice_in_dim(fluxes, 1, interior + 1, axis=along)


def sweep_adjoint(padded, courant_pad, along):
    interior = padded.shape[along] - 4

    def piece_of(first, last):
        return lax.slice_in_dim(padded, first, last, axis=along)

    differences = piece_of(2, interior + 4) - piece_of(1, interior + 3)
    scaled = courant_pad * differences
    return piece_of(2, interior + 2) + (2.0 * lax.slice_in_dim(scaled, 0, interior, axis=along) + 5.0 * lax.slice_in_dim(scaled, 1, interior + 1, axis=along) - lax.slice_in_dim(scaled, 2, interior + 2, axis=along)) / 6.0


def vertical_mix(field, mixing):
    fluxes = mixing * (field[1:] - field[:-1])
    zero_row = jnp.zeros_like(field[:1])
    return field + jnp.concatenate([fluxes, zero_row], axis=0) - jnp.concatenate([zero_row, fluxes], axis=0)


def horizontal(rimmed, wind_x, wind_y):
    swept = sweep_forward(rimmed, wind_x, 1)
    return sweep_forward(pad_periodic(swept, 2, 2), wind_y, 2)


def reference(checkpoint, adjoint_in, courant_x, courant_y, mixing, snd_column, snd_count, snd_step, snd_value, snd_weight, snd_kernel):
    device_total = N_GROUP * N_TILE
    wind_x = pad_periodic(courant_x, 1, 1)
    wind_y = pad_periodic(courant_y, 1, 2)
    tracer = jnp.roll(checkpoint, N_TILE * CX, axis=1)
    states = []
    for moment in range(STEPS):
        tracer = vertical_mix(horizontal(pad_periodic(tracer, 2, 1), wind_x, wind_y), mixing)
        states.append(tracer)
    shape_slots = (device_total, N_TILE, CAP)
    position = lax.broadcasted_iota(jnp.int32, shape_slots, 2)
    source_dev = lax.broadcasted_iota(jnp.int32, shape_slots, 0)
    target_tile = lax.broadcasted_iota(jnp.int32, shape_slots, 1)
    owner_dev = (source_dev // N_TILE) * N_TILE + target_tile
    cell_index = (owner_dev * (CX * CY) + snd_column).astype(jnp.int32).reshape(-1)
    weight = jnp.where(position < snd_count[:, :, None], snd_weight, jnp.zeros_like(snd_weight))
    kernels = snd_kernel.astype(jnp.float32)
    forcings = []
    for moment in range(STEPS):
        flattened = states[moment].reshape(LEV, -1)
        picked = jnp.take(flattened, cell_index, axis=1).reshape(LEV, device_total, N_TILE, CAP)
        observed = jnp.einsum("ldtc,dtlc->dtc", picked, kernels, precision=lax.Precision.HIGHEST)
        misfit = jnp.where(snd_step == moment, weight * (observed - snd_value), jnp.zeros_like(observed))
        contribution = jnp.einsum("dtlc,dtc->ldtc", kernels, misfit, precision=lax.Precision.HIGHEST).reshape(LEV, -1)
        forcing = jnp.zeros((LEV, NX * CY), jnp.float32).at[:, cell_index].add(contribution)
        forcings.append(forcing.reshape(LEV, NX, CY))
    adjoint = adjoint_in
    for moment in reversed(range(STEPS)):
        adjoint = vertical_mix(adjoint + forcings[moment], mixing)
        adjoint = sweep_adjoint(pad_periodic(adjoint, 2, 2), wind_y, 2)
        adjoint = sweep_adjoint(pad_periodic(adjoint, 2, 1), wind_x, 1)
    return adjoint
```

```python
import jax
import jax.numpy as jnp
from jax import lax
from jax.experimental import pallas as pl
from jax.experimental.pallas import tpu as pltpu
from jax.sharding import PartitionSpec as P

STEPS = 2


def padded_2(x, sides, width):
    edges = {}
    for axis, dim in sides:
        count, length = (lax.axis_size(axis), x.shape[dim])
        up = [(i, (i + 1) % count) for i in range(count)]
        last = lax.slice_in_dim(x, length - width, length, axis=dim)
        initial = lax.slice_in_dim(x, 0, width, axis=dim)
        edges[dim] = (
            lax.ppermute(last, axis, up),
            lax.ppermute(initial, axis, [(b, a) for a, b in up]),
        )
    done = []
    for _, dim in sides:
        low, high = edges[dim]
        around = [(width, width) if d in done else (0, 0) for d in range(x.ndim)]
        x = jnp.concatenate([jnp.pad(low, around), x, jnp.pad(high, around)], axis=dim)
        done.append(dim)
    return x


def from_behind(block, axis, distance):
    devices = range(lax.axis_size(axis))
    route = [((i - distance) % len(devices), i) for i in devices]
    return lax.ppermute(block, axis, route)


def with_halo(block, sides, width):
    for axis, dim in sides:
        count = lax.axis_size(axis)
        forward = [(i, i + 1) for i in range(count - 1)]
        forward.append((count - 1, 0))
        backward = [(target, source) for source, target in forward]
        low = lax.ppermute(
            lax.slice_in_dim(block, block.shape[dim] - width, None, axis=dim), axis, forward
        )
        high = lax.ppermute(lax.slice_in_dim(block, 0, width, axis=dim), axis, backward)
        block = jnp.concatenate([low, block, high], axis=dim)
    return block


def pad_periodic(field, width, along):
    total = field.shape[along]
    return jnp.concatenate(
        [
            lax.slice_in_dim(field, total - width, total, axis=along),
            field,
            lax.slice_in_dim(field, 0, width, axis=along),
        ],
        axis=along,
    )


def sweep_forward(padded, courant_pad, along):
    interior = padded.shape[along] - 4

    def piece_of(first, last):
        return lax.slice_in_dim(padded, first, last, axis=along)

    courant_face = lax.slice_in_dim(courant_pad, 0, interior + 1, axis=along)
    fluxes = (
        courant_face
        * (
            2.0 * piece_of(2, interior + 3)
            + 5.0 * piece_of(1, interior + 2)
            - piece_of(0, interior + 1)
        )
        / 6.0
    )
    return (
        piece_of(2, interior + 2)
        + lax.slice_in_dim(fluxes, 0, interior, axis=along)
        - lax.slice_in_dim(fluxes, 1, interior + 1, axis=along)
    )


def sweep_adjoint(padded, courant_pad, along):
    interior = padded.shape[along] - 4

    def piece_of(first, last):
        return lax.slice_in_dim(padded, first, last, axis=along)

    differences = piece_of(2, interior + 4) - piece_of(1, interior + 3)
    scaled = courant_pad * differences
    return (
        piece_of(2, interior + 2)
        + (
            2.0 * lax.slice_in_dim(scaled, 0, interior, axis=along)
            + 5.0 * lax.slice_in_dim(scaled, 1, interior + 1, axis=along)
            - lax.slice_in_dim(scaled, 2, interior + 2, axis=along)
        )
        / 6.0
    )


def vertical_mix(field, mixing):
    fluxes = mixing * (field[1:] - field[:-1])
    zero_row = jnp.zeros_like(field[:1])
    return (
        field
        + jnp.concatenate([fluxes, zero_row], axis=0)
        - jnp.concatenate([zero_row, fluxes], axis=0)
    )


def horizontal(rimmed, wind_x, wind_y):
    swept = sweep_forward(rimmed, wind_x, 1)
    return sweep_forward(pad_periodic(swept, 2, 2), wind_y, 2)


SLOT_ROWS = 1536


def sounding_kernel(row_ref, state_0, state_1, box, forcing_0, forcing_1, table, taken, spread, *sums):
    tiles = box.shape[0]

    def to_rows(i, carry):
        off = pl.multiple_of(i * 128, 128)
        for s, ref in enumerate((state_0, state_1)):
            for h in range(2):
                block = ref[:, h * 8 : h * 8 + 8, pl.ds(off, 128)].reshape(128, 128)
                at = pl.multiple_of(s * SLOT_ROWS + h * 768 + off, 128)
                table[pl.ds(at, 128), :] = block.T
        return carry

    lax.fori_loop(0, 6, to_rows, 0)

    def clear(i, carry):
        for acc in sums:
            acc[pl.ds(pl.multiple_of(i * 128, 128), 128), :] = jnp.zeros((128, 128), jnp.float32)
        return carry

    lax.fori_loop(0, 24, clear, 0)

    def gather(t, carry):
        base = pl.multiple_of(t * 128, 128)
        for k in range(128):
            taken[pl.ds(base + k, 1), :] = table[pl.ds(row_ref[base + k], 1), :]
        return carry

    lax.fori_loop(0, tiles, gather, 0)
    sub = lax.broadcasted_iota(jnp.int32, (8, 128), 0)

    def observe(t, carry):
        at = pl.ds(pl.multiple_of(t * 128, 128), 128)
        cells = taken[at, :].T
        rows = [box[t, :, f * 128 : f * 128 + 128] for f in range(18)]
        total = cells[0:8, :] * rows[0]
        for level in range(1, 16):
            total = total + cells[level * 8 : level * 8 + 8, :] * rows[level]
        lane = rows[17].astype(jnp.int32)
        own = sub == (lane // 768) % 8
        observed = jnp.sum(jnp.where(own, total, 0.0), axis=0, keepdims=True)
        misfit = jnp.where(own, jnp.broadcast_to(observed - rows[16], (8, 128)), 0.0)
        out = jnp.concatenate([misfit * rows[level] for level in range(16)], axis=0)
        spread[at, :] = out.T
        return carry

    lax.fori_loop(0, tiles, observe, 0)

    def scatter(t, carry):
        base = pl.multiple_of(t * 128, 128)
        for k in range(128):
            acc = sums[k % len(sums)]
            at = pl.ds(row_ref[base + k], 1)
            acc[at, :] = acc[at, :] + spread[pl.ds(base + k, 1), :]
        return carry

    lax.fori_loop(0, tiles, scatter, 0)

    def back(i, carry):
        off = pl.multiple_of(i * 128, 128)
        for s, ref in enumerate((forcing_0, forcing_1)):
            for h in range(2):
                at = pl.ds(pl.multiple_of(s * SLOT_ROWS + h * 768 + off, 128), 128)
                block = sums[0][at, :]
                for acc in sums[1:]:
                    block = block + acc[at, :]
                ref[:, h * 8 : h * 8 + 8, pl.ds(off, 128)] = block.T.reshape(16, 8, 128)
        return carry

    lax.fori_loop(0, 6, back, 0)


def forcings_of(row, state_0, state_1, box):
    vmem = pl.BlockSpec(memory_space=pltpu.VMEM)
    slots = box.shape[0] * 128
    return pl.pallas_call(
        sounding_kernel,
        out_shape=(jax.ShapeDtypeStruct(state_0.shape, jnp.float32),) * 2,
        in_specs=[pl.BlockSpec(memory_space=pltpu.SMEM), vmem, vmem, vmem],
        out_specs=(vmem, vmem),
        scratch_shapes=[pltpu.VMEM((2 * SLOT_ROWS, 128), jnp.float32)]
        + [pltpu.VMEM((slots, 128), jnp.float32)] * 2
        + [pltpu.VMEM((2 * SLOT_ROWS, 128), jnp.float32)] * 8,
        compiler_params=pltpu.CompilerParams(vmem_limit_bytes=48 * 2**20),
    )(row, state_0, state_1, box)


def on_device(
    checkpoint,
    adjoint_in,
    courant_x,
    courant_y,
    mixing,
    snd_column,
    snd_count,
    snd_step,
    snd_value,
    snd_weight,
    snd_kernel,
):
    levels, width_x, width_y = checkpoint.shape
    tile_count = snd_column.shape[1]
    capacity = snd_column.shape[2]
    wind_x = padded_2(courant_x, ((("group", "tile"), 1),), 1)
    wind_y = pad_periodic(courant_y, 1, 2)
    tracer = from_behind(checkpoint, "group", 1)
    rimmed = padded_2(tracer, ((("group", "tile"), 1),), 2)
    tracer = vertical_mix(horizontal(rimmed, wind_x, wind_y), mixing)
    states = [tracer]
    moment = 1
    rimmed = padded_2(tracer, ((("group", "tile"), 1),), 2)
    tracer = vertical_mix(horizontal(rimmed, wind_x, wind_y), mixing)
    states.append(tracer)
    position = lax.broadcasted_iota(jnp.int32, snd_column.shape, 2)
    weight = jnp.where(position < snd_count[:, :, None], snd_weight, jnp.zeros_like(snd_weight))
    root = jnp.sqrt(weight)
    packed = jnp.concatenate(
        [
            (snd_kernel * root[:, :, None, :]).reshape(tile_count, 1, levels * capacity),
            (snd_value * root).reshape(tile_count, 1, capacity),
            snd_column.astype(jnp.float32).reshape(tile_count, 1, capacity),
            snd_step.astype(jnp.float32).reshape(tile_count, 1, capacity),
        ],
        axis=2,
    )
    box = lax.all_to_all(packed, "tile", split_axis=0, concat_axis=0, tiled=True)
    fields = box.reshape(tile_count, -1)
    column = fields[:, 17 * capacity : 18 * capacity].astype(jnp.int32)
    step = fields[:, 18 * capacity :].astype(jnp.int32)
    row = step * SLOT_ROWS + column // (8 * width_y) * width_y + column % width_y
    forcings = forcings_of(row.reshape(-1), states[0], states[1], box)
    adjoint = adjoint_in
    for moment in reversed(range(STEPS)):
        adjoint = vertical_mix(adjoint + forcings[moment], mixing)
        adjoint = sweep_adjoint(pad_periodic(adjoint, 2, 2), wind_y, 2)
        rimmed = with_halo(adjoint, ((("group", "tile"), 1),), 2)
        adjoint = sweep_adjoint(rimmed, wind_x, 1)
    return adjoint


def solution(mesh):
    return jax.shard_map(
        on_device,
        mesh=mesh,
        in_specs=(
            P(None, ("group", "tile"), None),
            P(None, ("group", "tile"), None),
            P(None, ("group", "tile"), None),
            P(None, ("group", "tile"), None),
            P(None, ("group", "tile"), None),
            P(("group", "tile"), None, None),
            P(("group", "tile"), None),
            P(("group", "tile"), None, None),
            P(("group", "tile"), None, None),
            P(("group", "tile"), None, None),
            P(("group", "tile"), None, None, None),
        ),
        out_specs=P(None, ("group", "tile"), None),
        check_vma=False,
    )
```

```python
import jax
import jax.numpy as jnp
from jax import lax
from jax.experimental import pallas as pl
from jax.experimental.pallas import tpu as pltpu
from jax.sharding import PartitionSpec as P


RING = ("group", "tile")
SLOT_ROWS = 1536
UNROLL = 4


def shifted(block, distance):
    total = lax.axis_size(RING)
    return lax.ppermute(block, RING, [(i, (i + distance) % total) for i in range(total)])


def flux_y(v, courant):
    width, axis = v.shape[-1], v.ndim - 1
    ahead, behind = pltpu.roll(v, width - 1, axis), pltpu.roll(v, 1, axis)
    f = courant * (2.0 * ahead + 5.0 * v - behind) * (1.0 / 6.0)
    return v + pltpu.roll(f, 1, axis) - f


def sweep_y(a, courant):
    width, axis = a.shape[-1], a.ndim - 1
    g = courant * (pltpu.roll(a, width - 1, axis) - a)
    return a + (2.0 * pltpu.roll(g, 1, axis) + 5.0 * g - pltpu.roll(g, width - 1, axis)) * (1.0 / 6.0)


def mix_rows(c, mixing):
    levels = c.shape[0]
    f = mixing * (pltpu.roll(c, levels - 1, 0) - c)
    return c + f - pltpu.roll(f, 1, 0)


def mixing_row(mixing, x):
    row = mixing[:, x, :]
    return jnp.concatenate([row, jnp.zeros((1, row.shape[1]), row.dtype)], axis=0)


def sounding_kernel(
    table,
    box,
    far_adjoint,
    far_courant_x,
    far_courant_y,
    far_mixing,
    forcing_0,
    swept_1,
    to_low,
    to_high,
    courant_x,
    courant_y,
    mixing,
    adjoint_in,
    field_done,
    forcing_1,
    row_wide,
    row_ref,
    row_done,
    taken_0,
    taken_1,
    spread_0,
    spread_1,
    *sums,
):
    tiles = box.shape[0]
    width_y = adjoint_in.shape[2]

    def rows_of(t, carry):
        column = box[t, :, 17 * 128 : 18 * 128].astype(jnp.int32)
        step = box[t, :, 18 * 128 :].astype(jnp.int32)
        row = step * SLOT_ROWS + column // (8 * width_y) * width_y + column % width_y
        row_wide[pl.ds(t, 1), :] = row
        return carry

    lax.fori_loop(0, tiles, rows_of, 0, unroll=8)
    copy_rows = pltpu.make_async_copy(row_wide, row_ref, row_done)
    copy_rows.start()
    pairs = (
        (far_adjoint, adjoint_in),
        (far_courant_x, courant_x),
        (far_courant_y, courant_y),
        (far_mixing, mixing),
    )
    copies = [pltpu.make_async_copy(*pair, field_done.at[n]) for n, pair in enumerate(pairs)]
    for copy in copies:
        copy.start()

    def clear(i, carry):
        for acc in sums:
            acc[pl.ds(pl.multiple_of(i * 128, 128), 128), :] = jnp.zeros((128, 128), jnp.float32)
        return carry

    lax.fori_loop(0, 24, clear, 0)
    copy_rows.wait()

    sub = lax.broadcasted_iota(jnp.int32, (8, 128), 0)

    def gather(t, taken):
        for k in range(128):
            taken[k : k + 1, :] = table[pl.ds(row_ref[t, k], 1), :]

    def observe(t, taken, spread):
        cells = taken[...].T
        rows = [box[t, :, f * 128 : f * 128 + 128] for f in range(18)]
        total = cells[0:8, :] * rows[0]
        for level in range(1, 16):
            total = total + cells[level * 8 : level * 8 + 8, :] * rows[level]
        own = sub == (rows[17].astype(jnp.int32) // 768) % 8
        observed = jnp.sum(jnp.where(own, total, 0.0), axis=0, keepdims=True)
        misfit = jnp.where(own, jnp.broadcast_to(observed - rows[16], (8, 128)), 0.0)
        spread[...] = jnp.concatenate([misfit * rows[level] for level in range(16)], axis=0).T

    def scatter(t, spread):
        for k in range(128):
            acc = sums[k % len(sums)]
            at = pl.ds(row_ref[t, k], 1)
            acc[at, :] = acc[at, :] + spread[k : k + 1, :]

    spread_1[...] = jnp.zeros((128, 128), jnp.float32)
    gather(0, taken_0)

    def two(i, carry):
        t = 2 * i
        observe(t, taken_0, spread_0)
        gather(t + 1, taken_1)
        scatter(jnp.maximum(t - 1, 0), spread_1)
        observe(t + 1, taken_1, spread_1)
        gather(jnp.minimum(t + 2, tiles - 1), taken_0)
        scatter(t, spread_0)
        return carry

    lax.fori_loop(0, tiles // 2, two, 0)
    scatter(tiles - 1, spread_1)

    def back(i, carry):
        off = pl.multiple_of(i * 128, 128)
        for s, ref in enumerate((forcing_0, forcing_1)):
            for h in range(2):
                at = pl.ds(pl.multiple_of(s * SLOT_ROWS + h * 768 + off, 128), 128)
                block = sums[0][at, :]
                for acc in sums[1:]:
                    block = block + acc[at, :]
                ref[:, h * 8 : h * 8 + 8, pl.ds(off, 128)] = block.T.reshape(16, 8, 128)
        return carry

    lax.fori_loop(0, 6, back, 0)
    levels = adjoint_in.shape[0]
    for copy in copies:
        copy.wait()

    def first_step(level, carry):
        here, below = carry
        above = jnp.minimum(level + 1, levels - 1)
        upper = adjoint_in[above] + forcing_1[above]
        flux = mixing[jnp.minimum(level, levels - 2)] * (upper - here)
        flux = jnp.where(level < levels - 1, flux, 0.0)
        swept_1[level] = sweep_y(here + flux - below, courant_y[level])
        return upper, flux

    start = adjoint_in[0] + forcing_1[0]
    lax.fori_loop(0, levels, first_step, (start, jnp.zeros_like(start)), unroll=UNROLL)
    b = {x: swept_1[:, x, :] for x in (0, 1, 2, 3, 14, 15)}
    g = {x: courant_x[:, x, :] * (b[x + 1] - b[x]) for x in (0, 1, 2, 14)}
    to_low[0] = b[0]
    to_low[1] = g[0]
    to_low[2] = b[0] + (5.0 * g[0] - g[1]) * (1.0 / 6.0) + forcing_0[:, 0, :]
    a = b[1] + (2.0 * g[0] + 5.0 * g[1] - g[2]) * (1.0 / 6.0) + forcing_0[:, 1, :]
    to_low[3] = sweep_y(mix_rows(a, mixing_row(mixing, 1)), courant_y[:, 1, :])
    to_high[0] = b[15]
    to_high[1] = b[15] + g[14] * (1.0 / 3.0) + forcing_0[:, 15, :]


def adjoint_to_edges(table, box, adjoint_in, *winds):
    vmem, hbm = (pl.BlockSpec(memory_space=space) for space in (pltpu.VMEM, pltpu.HBM))
    levels, _, width_y = adjoint_in.shape
    edges = tuple(jax.ShapeDtypeStruct((n, levels, width_y), jnp.float32) for n in (4, 2))
    return pl.pallas_call(
        sounding_kernel,
        out_shape=shapes_of(adjoint_in, adjoint_in) + edges + shapes_of(*winds),
        in_specs=[vmem] * 2 + [hbm] * 4,
        out_specs=(vmem,) * 7,
        scratch_shapes=[
            pltpu.VMEM(adjoint_in.shape, jnp.float32),
            pltpu.SemaphoreType.DMA((4,)),
            pltpu.VMEM(adjoint_in.shape, jnp.float32),
            pltpu.VMEM((box.shape[0], 128), jnp.int32),
            pltpu.SMEM((box.shape[0], 128), jnp.int32),
            pltpu.SemaphoreType.DMA,
        ]
        + [pltpu.VMEM((128, 128), jnp.float32)] * 4
        + [pltpu.VMEM((2 * SLOT_ROWS, 128), jnp.float32)] * 8,
        compiler_params=pltpu.CompilerParams(vmem_limit_bytes=26 * 2**20),
    )(table, box, adjoint_in, *winds)


def final_kernel(
    swept_1, forcing_0, courant_x, courant_y, mixing, low, high, rim_low, rim_high, out, edges
):
    levels, width_x = swept_1.shape[:2]
    wind_low, wind_high = rim_low.at[4:7], rim_high.at[2:5]
    sixth = 1.0 / 6.0
    b_first, b_next, b_last = swept_1[:, 0, :], swept_1[:, 1, :], swept_1[:, width_x - 1, :]
    g_low = wind_low[0] * (b_first - low[0])
    g_first = courant_x[:, 0, :] * (b_next - b_first)
    g_last = courant_x[:, width_x - 1, :] * (high[0] - b_last)
    before = sweep_y(mix_rows(low[1] + (5.0 * g_low - g_first) * sixth, wind_low[2]), wind_low[1])
    after = sweep_y(mix_rows(high[2] + g_last * (1.0 / 3.0), wind_high[2]), wind_high[1])
    edges[0] = g_low
    edges[1] = before
    edges[2] = after
    edges[3] = wind_high[0] * (high[3] - after)
    sub = lax.broadcasted_iota(jnp.int32, swept_1.shape[1:], 0)

    def up(field, row):
        return jnp.where(sub == width_x - 1, row, pltpu.roll(field, width_x - 1, 0))

    def down(field, row):
        return jnp.where(sub == 0, row, pltpu.roll(field, 1, 0))

    def sweep_x(field, courant, after_last, g_before, g_after):
        g = courant * (up(field, after_last) - field)
        return field + (2.0 * down(g, g_before) + 5.0 * g - up(g, g_after)) * sixth

    def entering(level):
        at = pl.ds(level, 1)
        swept = sweep_x(
            swept_1[level], courant_x[level], high[0, at, :], edges[0, at, :], high[1, at, :]
        )
        return swept + forcing_0[level]

    def second_step(level, carry):
        here, below = carry
        at = pl.ds(level, 1)
        upper = entering(jnp.minimum(level + 1, levels - 1))
        flux = mixing[jnp.minimum(level, levels - 2)] * (upper - here)
        flux = jnp.where(level < levels - 1, flux, 0.0)
        b = sweep_y(here + flux - below, courant_y[level])
        c = courant_x[level]
        g_before = wind_low[0, at, :] * (b[0:1, :] - edges[1, at, :])
        out[level] = sweep_x(b, c, edges[2, at, :], g_before, edges[3, at, :])
        return upper, flux

    start = entering(0)
    lax.fori_loop(0, levels, second_step, (start, jnp.zeros_like(start)), unroll=UNROLL)


def adjoint_final(*fields):
    vmem = pl.BlockSpec(memory_space=pltpu.VMEM)
    shape = fields[0].shape
    return pl.pallas_call(
        final_kernel,
        out_shape=jax.ShapeDtypeStruct(shape, jnp.float32),
        in_specs=[vmem] * len(fields),
        out_specs=vmem,
        scratch_shapes=[pltpu.VMEM((4, shape[0], shape[2]), jnp.float32)],
        compiler_params=pltpu.CompilerParams(vmem_limit_bytes=4 * 2**20),
    )(*fields)


def pack_soundings(snd_column, snd_count, snd_step, snd_value, snd_weight, snd_kernel):
    _, tile_count, _ = snd_column.shape
    position = lax.broadcasted_iota(jnp.int32, snd_column.shape, 2)
    weight = jnp.where(position < snd_count[:, :, None], snd_weight, jnp.zeros_like(snd_weight))
    root = jnp.sqrt(weight)
    parts = (
        snd_kernel * root[:, :, None, :],
        snd_value * root,
        snd_column.astype(jnp.float32),
        snd_step.astype(jnp.float32),
    )
    return jnp.concatenate([p.reshape(tile_count, 1, -1) for p in parts], axis=2)


def rim_kernel(*refs):
    sources, (to_high, to_low), local, done = refs[:3], refs[4:6], refs[6:9], refs[9]
    tracer = refs[3]
    copies = [
        pltpu.make_async_copy(source, target, done.at[n])
        for n, (source, target) in enumerate(zip(sources, local))
    ]
    for copy in copies:
        copy.start()
    for copy in copies:
        copy.wait()
    courant_x, courant_y, mixing = local
    last = tracer.shape[1] - 1
    sixth = 1.0 / 6.0
    c = {x: tracer[:, x, :] for x in (0, 1, last - 3, last - 2, last - 1, last)}
    w = {x: courant_x[:, x, :] for x in (0, last - 2, last - 1, last)}

    def flux(x):
        return w[x] * (2.0 * c[x + 1] + 5.0 * c[x] - c[x - 1]) * sixth

    inner = flux(last - 1)
    swept = flux_y(c[last - 1] + flux(last - 2) - inner, courant_y[:, last - 1, :])
    to_high[0] = mix_rows(swept, mixing_row(mixing, last - 1))
    known = w[last] * (5.0 * c[last] - c[last - 1]) * sixth
    to_high[1] = c[last] + inner - known
    to_high[2] = known
    to_high[3] = c[last]
    to_low[0] = c[0]
    to_low[1] = c[0] - w[0] * (2.0 * c[1] + 5.0 * c[0]) * sixth
    for ref, first, x in ((to_high, 4, last), (to_low, 2, 0)):
        ref[first] = courant_x[:, x, :]
        ref[first + 1] = courant_y[:, x, :]
        ref[first + 2] = mixing_row(mixing, x)


def shapes_of(*fields):
    return tuple(jax.ShapeDtypeStruct(x.shape, x.dtype) for x in fields)


def rims(tracer, *winds):
    vmem = pl.BlockSpec(memory_space=pltpu.VMEM)
    levels, _, width_y = tracer.shape
    edges = tuple(jax.ShapeDtypeStruct((n, levels, width_y), jnp.float32) for n in (7, 5))
    return pl.pallas_call(
        rim_kernel,
        out_shape=edges + shapes_of(*winds),
        in_specs=[pl.BlockSpec(memory_space=pltpu.HBM)] * len(winds) + [vmem],
        out_specs=(vmem,) * 5,
        scratch_shapes=[pltpu.SemaphoreType.DMA((len(winds),))],
        compiler_params=pltpu.CompilerParams(vmem_limit_bytes=8 * 2**20),
    )(*winds, tracer)


def forward_kernel(tracer, low, high, courant_x, courant_y, mixing, table, first, second, edges):
    levels, width_x, width_y = tracer.shape
    sixth = 1.0 / 6.0
    last = width_x - 1
    sub = lax.broadcasted_iota(jnp.int32, tracer.shape[1:], 0)
    wind_low, wind_high = low[4], high[2]
    c_first, c_last = tracer[:, 0, :], tracer[:, last, :]
    reach = wind_low * c_first * (1.0 / 3.0)
    edges[0] = low[3]
    edges[1] = low[2] + reach
    edges[2] = high[0]
    near = mix_rows(flux_y(low[1] - reach, low[5]), low[6])
    flux_last = (
        courant_x[:, last, :] * (2.0 * high[0] + 5.0 * c_last - tracer[:, last - 1, :]) * sixth
    )
    after = flux_y(high[1] + wind_high * c_last * sixth + flux_last, high[3])
    edges[3] = near
    edges[5] = mix_rows(after, high[4])

    def step(source, target, e):
        def entering(level):
            at = pl.ds(level, 1)
            c, w = source[level], courant_x[level]
            ahead = jnp.where(sub == last, edges[e + 2, at, :], pltpu.roll(c, last, 0))
            behind = jnp.where(sub == 0, edges[e, at, :], pltpu.roll(c, 1, 0))
            f = w * (2.0 * ahead + 5.0 * c - behind) * sixth
            swept = c + jnp.where(sub == 0, edges[e + 1, at, :], pltpu.roll(f, 1, 0)) - f
            return flux_y(swept, courant_y[level])

        def one(level, carry):
            here, below = carry
            upper = entering(jnp.minimum(level + 1, levels - 1))
            flux = mixing[jnp.minimum(level, levels - 2)] * (upper - here)
            flux = jnp.where(level < levels - 1, flux, 0.0)
            target[level] = here + flux - below
            return upper, flux

        start = entering(0)
        lax.fori_loop(0, levels, one, (start, jnp.zeros_like(start)), unroll=UNROLL)

    step(tracer, first, 0)
    edges[4] = wind_low * (2.0 * first[:, 0, :] + 5.0 * near - low[0]) * sixth
    step(first, second, 3)

    def to_rows(i, carry):
        off = pl.multiple_of(i * 128, 128)
        for s, ref in enumerate((first, second)):
            for h in range(2):
                block = ref[:, h * 8 : h * 8 + 8, pl.ds(off, 128)].reshape(128, 128)
                at = pl.multiple_of(s * SLOT_ROWS + h * width_y + off, 128)
                table[pl.ds(at, 128), :] = block.T
        return carry

    lax.fori_loop(0, width_y // 128, to_rows, 0)


def forward(*fields):
    vmem = pl.BlockSpec(memory_space=pltpu.VMEM)
    shape = fields[0].shape
    return pl.pallas_call(
        forward_kernel,
        out_shape=jax.ShapeDtypeStruct((2 * SLOT_ROWS, 128), jnp.float32),
        in_specs=[vmem] * len(fields),
        out_specs=vmem,
        scratch_shapes=[pltpu.VMEM(shape, jnp.float32)] * 2
        + [pltpu.VMEM((6, shape[0], shape[2]), jnp.float32)],
        compiler_params=pltpu.CompilerParams(vmem_limit_bytes=6 * 2**20),
    )(*fields)


def program(
    checkpoint,
    adjoint_in,
    courant_x,
    courant_y,
    mixing,
    snd_column,
    snd_count,
    snd_step,
    snd_value,
    snd_weight,
    snd_kernel,
):
    tiles = snd_column.shape[1]
    *winds, adjoint_in = (
        pltpu.with_memory_space_constraint(x, pltpu.HBM)
        for x in (courant_x, courant_y, mixing, adjoint_in)
    )
    tracer = shifted(checkpoint, tiles)
    packed = pack_soundings(
        snd_column, snd_count, snd_step, snd_value, snd_weight, snd_kernel
    )
    box = lax.all_to_all(packed, "tile", split_axis=0, concat_axis=0, tiled=True)
    to_high, to_low, *near_winds = rims(tracer, *winds)
    low = shifted(to_high, 1)
    high = shifted(to_low, -1)
    table = forward(tracer, low, high, *near_winds)
    forcing_0, swept_1, to_low, to_high, *near_winds = adjoint_to_edges(
        table, box, adjoint_in, *winds
    )
    from_high = shifted(to_low, -1)
    from_low = shifted(to_high, 1)
    return adjoint_final(
        swept_1, forcing_0, *near_winds, from_low, from_high, low, high
    )


def solution(mesh):
    return jax.shard_map(
        program,
        mesh=mesh,
        in_specs=(P(None, RING, None),) * 5
        + (P(RING, None, None), P(RING, None))
        + (P(RING, None, None),) * 3
        + (P(RING, None, None, None),),
        out_specs=P(None, RING, None),
        check_vma=False,
    )
```

```python
import jax
import jax.numpy as jnp
from jax import lax
from jax.experimental import pallas as pl
from jax.experimental.pallas import tpu as pltpu
from jax.sharding import PartitionSpec as P


RING = ("group", "tile")
SLOT_ROWS = 1536
UNROLL = 4


def shifted(block, distance):
    total = lax.axis_size(RING)
    return lax.ppermute(block, RING, [(i, (i + distance) % total) for i in range(total)])


def flux_y(v, courant):
    width, axis = v.shape[-1], v.ndim - 1
    ahead, behind = pltpu.roll(v, width - 1, axis), pltpu.roll(v, 1, axis)
    f = courant * (2.0 * ahead + 5.0 * v - behind) * (1.0 / 6.0)
    return v + pltpu.roll(f, 1, axis) - f


def sweep_y(a, courant):
    width, axis = a.shape[-1], a.ndim - 1
    g = courant * (pltpu.roll(a, width - 1, axis) - a)
    return a + (2.0 * pltpu.roll(g, 1, axis) + 5.0 * g - pltpu.roll(g, width - 1, axis)) * (1.0 / 6.0)


def mix_rows(c, mixing):
    levels = c.shape[0]
    f = mixing * (pltpu.roll(c, levels - 1, 0) - c)
    return c + f - pltpu.roll(f, 1, 0)


def mixing_row(mixing, x):
    row = mixing[:, x, :]
    return jnp.concatenate([row, jnp.zeros((1, row.shape[1]), row.dtype)], axis=0)


def sounding_kernel(
    table,
    box,
    far_adjoint,
    far_courant_x,
    far_courant_y,
    far_mixing,
    forcing_0,
    swept_1,
    to_low,
    to_high,
    courant_x,
    courant_y,
    mixing,
    adjoint_in,
    field_done,
    forcing_1,
    row_wide,
    row_ref,
    row_done,
    taken_0,
    taken_1,
    spread_0,
    spread_1,
    *sums,
):
    tiles = box.shape[0]
    width_y = adjoint_in.shape[2]

    def rows_of(t, carry):
        column = box[t, :, 17 * 128 : 18 * 128].astype(jnp.int32)
        step = box[t, :, 18 * 128 :].astype(jnp.int32)
        row = step * SLOT_ROWS + column // (8 * width_y) * width_y + column % width_y
        row_wide[pl.ds(t, 1), :] = row
        return carry

    lax.fori_loop(0, tiles, rows_of, 0, unroll=8)
    copy_rows = pltpu.make_async_copy(row_wide, row_ref, row_done)
    copy_rows.start()
    pairs = (
        (far_adjoint, adjoint_in),
        (far_courant_x, courant_x),
        (far_courant_y, courant_y),
        (far_mixing, mixing),
    )
    copies = [pltpu.make_async_copy(*pair, field_done.at[n]) for n, pair in enumerate(pairs)]
    for copy in copies:
        copy.start()

    def clear(i, carry):
        for acc in sums:
            acc[pl.ds(pl.multiple_of(i * 128, 128), 128), :] = jnp.zeros((128, 128), jnp.float32)
        return carry

    lax.fori_loop(0, 24, clear, 0)
    copy_rows.wait()

    sub = lax.broadcasted_iota(jnp.int32, (8, 128), 0)

    def gather(t, taken):
        for k in range(128):
            taken[k : k + 1, :] = table[pl.ds(row_ref[t, k], 1), :]

    def observe(t, taken, spread):
        cells = taken[...].T
        rows = [box[t, :, f * 128 : f * 128 + 128] for f in range(18)]
        total = cells[0:8, :] * rows[0]
        for level in range(1, 16):
            total = total + cells[level * 8 : level * 8 + 8, :] * rows[level]
        own = sub == (rows[17].astype(jnp.int32) // 768) % 8
        observed = jnp.sum(jnp.where(own, total, 0.0), axis=0, keepdims=True)
        misfit = jnp.where(own, jnp.broadcast_to(observed - rows[16], (8, 128)), 0.0)
        spread[...] = jnp.concatenate([misfit * rows[level] for level in range(16)], axis=0).T

    def scatter(t, spread):
        for k in range(128):
            acc = sums[k % len(sums)]
            at = pl.ds(row_ref[t, k], 1)
            acc[at, :] = acc[at, :] + spread[k : k + 1, :]

    spread_1[...] = jnp.zeros((128, 128), jnp.float32)
    gather(0, taken_0)

    def two(i, carry):
        t = 2 * i
        observe(t, taken_0, spread_0)
        gather(t + 1, taken_1)
        scatter(jnp.maximum(t - 1, 0), spread_1)
        observe(t + 1, taken_1, spread_1)
        gather(jnp.minimum(t + 2, tiles - 1), taken_0)
        scatter(t, spread_0)
        return carry

    lax.fori_loop(0, tiles // 2, two, 0)
    scatter(tiles - 1, spread_1)

    def back(i, carry):
        off = pl.multiple_of(i * 128, 128)
        for s, ref in enumerate((forcing_0, forcing_1)):
            for h in range(2):
                at = pl.ds(pl.multiple_of(s * SLOT_ROWS + h * 768 + off, 128), 128)
                block = sums[0][at, :]
                for acc in sums[1:]:
                    block = block + acc[at, :]
                ref[:, h * 8 : h * 8 + 8, pl.ds(off, 128)] = block.T.reshape(16, 8, 128)
        return carry

    lax.fori_loop(0, 6, back, 0)
    levels = adjoint_in.shape[0]
    for copy in copies:
        copy.wait()

    def first_step(level, carry):
        here, below = carry
        above = jnp.minimum(level + 1, levels - 1)
        upper = adjoint_in[above] + forcing_1[above]
        flux = mixing[jnp.minimum(level, levels - 2)] * (upper - here)
        flux = jnp.where(level < levels - 1, flux, 0.0)
        swept_1[level] = sweep_y(here + flux - below, courant_y[level])
        return upper, flux

    start = adjoint_in[0] + forcing_1[0]
    lax.fori_loop(0, levels, first_step, (start, jnp.zeros_like(start)), unroll=UNROLL)
    b = {x: swept_1[:, x, :] for x in (0, 1, 2, 3, 14, 15)}
    g = {x: courant_x[:, x, :] * (b[x + 1] - b[x]) for x in (0, 1, 2, 14)}
    to_low[0] = b[0]
    to_low[1] = g[0]
    to_low[2] = b[0] + (5.0 * g[0] - g[1]) * (1.0 / 6.0) + forcing_0[:, 0, :]
    a = b[1] + (2.0 * g[0] + 5.0 * g[1] - g[2]) * (1.0 / 6.0) + forcing_0[:, 1, :]
    to_low[3] = sweep_y(mix_rows(a, mixing_row(mixing, 1)), courant_y[:, 1, :])
    to_high[0] = b[15]
    to_high[1] = b[15] + g[14] * (1.0 / 3.0) + forcing_0[:, 15, :]


def adjoint_to_edges(table, box, adjoint_in, *winds):
    vmem, hbm = (pl.BlockSpec(memory_space=space) for space in (pltpu.VMEM, pltpu.HBM))
    levels, _, width_y = adjoint_in.shape
    edges = tuple(jax.ShapeDtypeStruct((n, levels, width_y), jnp.float32) for n in (4, 2))
    return pl.pallas_call(
        sounding_kernel,
        out_shape=shapes_of(adjoint_in, adjoint_in) + edges + shapes_of(*winds),
        in_specs=[vmem] * 2 + [hbm] * 4,
        out_specs=(vmem,) * 7,
        scratch_shapes=[
            pltpu.VMEM(adjoint_in.shape, jnp.float32),
            pltpu.SemaphoreType.DMA((4,)),
            pltpu.VMEM(adjoint_in.shape, jnp.float32),
            pltpu.VMEM((box.shape[0], 128), jnp.int32),
            pltpu.SMEM((box.shape[0], 128), jnp.int32),
            pltpu.SemaphoreType.DMA,
        ]
        + [pltpu.VMEM((128, 128), jnp.float32)] * 4
        + [pltpu.VMEM((2 * SLOT_ROWS, 128), jnp.float32)] * 8,
        compiler_params=pltpu.CompilerParams(vmem_limit_bytes=26 * 2**20),
    )(table, box, adjoint_in, *winds)


def final_kernel(
    swept_1, forcing_0, courant_x, courant_y, mixing, low, high, rim_low, rim_high, out, edges
):
    levels, width_x = swept_1.shape[:2]
    wind_low, wind_high = rim_low.at[4:7], rim_high.at[2:5]
    sixth = 1.0 / 6.0
    b_first, b_next, b_last = swept_1[:, 0, :], swept_1[:, 1, :], swept_1[:, width_x - 1, :]
    g_low = wind_low[0] * (b_first - low[0])
    g_first = courant_x[:, 0, :] * (b_next - b_first)
    g_last = courant_x[:, width_x - 1, :] * (high[0] - b_last)
    before = sweep_y(mix_rows(low[1] + (5.0 * g_low - g_first) * sixth, wind_low[2]), wind_low[1])
    after = sweep_y(mix_rows(high[2] + g_last * (1.0 / 3.0), wind_high[2]), wind_high[1])
    edges[0] = g_low
    edges[1] = before
    edges[2] = after
    edges[3] = wind_high[0] * (high[3] - after)
    sub = lax.broadcasted_iota(jnp.int32, swept_1.shape[1:], 0)

    def up(field, row):
        return jnp.where(sub == width_x - 1, row, pltpu.roll(field, width_x - 1, 0))

    def down(field, row):
        return jnp.where(sub == 0, row, pltpu.roll(field, 1, 0))

    def sweep_x(field, courant, after_last, g_before, g_after):
        g = courant * (up(field, after_last) - field)
        return field + (2.0 * down(g, g_before) + 5.0 * g - up(g, g_after)) * sixth

    def entering(level):
        at = pl.ds(level, 1)
        swept = sweep_x(
            swept_1[level], courant_x[level], high[0, at, :], edges[0, at, :], high[1, at, :]
        )
        return swept + forcing_0[level]

    def second_step(level, carry):
        here, below = carry
        at = pl.ds(level, 1)
        upper = entering(jnp.minimum(level + 1, levels - 1))
        flux = mixing[jnp.minimum(level, levels - 2)] * (upper - here)
        flux = jnp.where(level < levels - 1, flux, 0.0)
        b = sweep_y(here + flux - below, courant_y[level])
        c = courant_x[level]
        g_before = wind_low[0, at, :] * (b[0:1, :] - edges[1, at, :])
        out[level] = sweep_x(b, c, edges[2, at, :], g_before, edges[3, at, :])
        return upper, flux

    start = entering(0)
    lax.fori_loop(0, levels, second_step, (start, jnp.zeros_like(start)), unroll=UNROLL)


def adjoint_final(*fields):
    vmem = pl.BlockSpec(memory_space=pltpu.VMEM)
    shape = fields[0].shape
    return pl.pallas_call(
        final_kernel,
        out_shape=jax.ShapeDtypeStruct(shape, jnp.float32),
        in_specs=[vmem] * len(fields),
        out_specs=vmem,
        scratch_shapes=[pltpu.VMEM((4, shape[0], shape[2]), jnp.float32)],
        compiler_params=pltpu.CompilerParams(vmem_limit_bytes=4 * 2**20),
    )(*fields)


def pack_kernel(count, *refs):
    sources, packed, local, root, done = refs[:5], refs[5], refs[6:11], refs[11], refs[12]
    copies = [
        pltpu.make_async_copy(source, target, done.at[n])
        for n, (source, target) in enumerate(zip(sources, local))
    ]
    for copy in copies:
        copy.start()
    column, step, value, weight, kernel = local
    tiles, capacity = column.shape[1:]
    levels = kernel.shape[2]
    position = lax.broadcasted_iota(jnp.int32, (1, capacity), 1)
    for copy in copies:
        copy.wait()
    for t in range(tiles):
        root[t : t + 1, :] = jnp.where(position < count[0, t], weight[0, t : t + 1, :], 0.0)
    root[...] = jnp.sqrt(root[...])

    def one(t, carry):
        at = pl.ds(t, 1)
        scale = root[at, :]
        rows = kernel[0, t] * scale
        for level in range(levels):
            packed[t, :, level * capacity : (level + 1) * capacity] = rows[level : level + 1, :]
        rest = (
            value[0, at, :] * scale,
            column[0, at, :].astype(jnp.float32),
            step[0, at, :].astype(jnp.float32),
        )
        for f, part in enumerate(rest, levels):
            packed[t, :, f * capacity : (f + 1) * capacity] = part
        return carry

    lax.fori_loop(0, tiles, one, 0, unroll=4)


def pack(count, *fields):
    _, tiles, levels, capacity = fields[4].shape
    vmem, hbm = (pl.BlockSpec(memory_space=space) for space in (pltpu.VMEM, pltpu.HBM))
    return pl.pallas_call(
        pack_kernel,
        out_shape=jax.ShapeDtypeStruct((tiles, 1, (levels + 3) * capacity), jnp.float32),
        in_specs=[pl.BlockSpec(memory_space=pltpu.SMEM)] + [hbm] * len(fields),
        out_specs=vmem,
        scratch_shapes=[pltpu.VMEM(x.shape, x.dtype) for x in fields]
        + [
            pltpu.VMEM((tiles, capacity), jnp.float32),
            pltpu.SemaphoreType.DMA((len(fields),)),
        ],
        compiler_params=pltpu.CompilerParams(vmem_limit_bytes=4 * 2**20),
    )(count, *fields)


def rim_kernel(*refs):
    sources, (to_high, to_low), local, done = refs[:3], refs[4:6], refs[6:9], refs[9]
    tracer = refs[3]
    copies = [
        pltpu.make_async_copy(source, target, done.at[n])
        for n, (source, target) in enumerate(zip(sources, local))
    ]
    for copy in copies:
        copy.start()
    for copy in copies:
        copy.wait()
    courant_x, courant_y, mixing = local
    last = tracer.shape[1] - 1
    sixth = 1.0 / 6.0
    c = {x: tracer[:, x, :] for x in (0, 1, last - 3, last - 2, last - 1, last)}
    w = {x: courant_x[:, x, :] for x in (0, last - 2, last - 1, last)}

    def flux(x):
        return w[x] * (2.0 * c[x + 1] + 5.0 * c[x] - c[x - 1]) * sixth

    inner = flux(last - 1)
    swept = flux_y(c[last - 1] + flux(last - 2) - inner, courant_y[:, last - 1, :])
    to_high[0] = mix_rows(swept, mixing_row(mixing, last - 1))
    known = w[last] * (5.0 * c[last] - c[last - 1]) * sixth
    to_high[1] = c[last] + inner - known
    to_high[2] = known
    to_high[3] = c[last]
    to_low[0] = c[0]
    to_low[1] = c[0] - w[0] * (2.0 * c[1] + 5.0 * c[0]) * sixth
    for ref, first, x in ((to_high, 4, last), (to_low, 2, 0)):
        ref[first] = courant_x[:, x, :]
        ref[first + 1] = courant_y[:, x, :]
        ref[first + 2] = mixing_row(mixing, x)


def shapes_of(*fields):
    return tuple(jax.ShapeDtypeStruct(x.shape, x.dtype) for x in fields)


def rims(tracer, *winds):
    vmem = pl.BlockSpec(memory_space=pltpu.VMEM)
    levels, _, width_y = tracer.shape
    edges = tuple(jax.ShapeDtypeStruct((n, levels, width_y), jnp.float32) for n in (7, 5))
    return pl.pallas_call(
        rim_kernel,
        out_shape=edges + shapes_of(*winds),
        in_specs=[pl.BlockSpec(memory_space=pltpu.HBM)] * len(winds) + [vmem],
        out_specs=(vmem,) * 5,
        scratch_shapes=[pltpu.SemaphoreType.DMA((len(winds),))],
        compiler_params=pltpu.CompilerParams(vmem_limit_bytes=8 * 2**20),
    )(*winds, tracer)


def forward_kernel(tracer, low, high, courant_x, courant_y, mixing, table, first, second, edges):
    levels, width_x, width_y = tracer.shape
    sixth = 1.0 / 6.0
    last = width_x - 1
    sub = lax.broadcasted_iota(jnp.int32, tracer.shape[1:], 0)
    wind_low, wind_high = low[4], high[2]
    c_first, c_last = tracer[:, 0, :], tracer[:, last, :]
    reach = wind_low * c_first * (1.0 / 3.0)
    edges[0] = low[3]
    edges[1] = low[2] + reach
    edges[2] = high[0]
    near = mix_rows(flux_y(low[1] - reach, low[5]), low[6])
    flux_last = (
        courant_x[:, last, :] * (2.0 * high[0] + 5.0 * c_last - tracer[:, last - 1, :]) * sixth
    )
    after = flux_y(high[1] + wind_high * c_last * sixth + flux_last, high[3])
    edges[3] = near
    edges[5] = mix_rows(after, high[4])

    def step(source, target, e):
        def entering(level):
            at = pl.ds(level, 1)
            c, w = source[level], courant_x[level]
            ahead = jnp.where(sub == last, edges[e + 2, at, :], pltpu.roll(c, last, 0))
            behind = jnp.where(sub == 0, edges[e, at, :], pltpu.roll(c, 1, 0))
            f = w * (2.0 * ahead + 5.0 * c - behind) * sixth
            swept = c + jnp.where(sub == 0, edges[e + 1, at, :], pltpu.roll(f, 1, 0)) - f
            return flux_y(swept, courant_y[level])

        def one(level, carry):
            here, below = carry
            upper = entering(jnp.minimum(level + 1, levels - 1))
            flux = mixing[jnp.minimum(level, levels - 2)] * (upper - here)
            flux = jnp.where(level < levels - 1, flux, 0.0)
            target[level] = here + flux - below
            return upper, flux

        start = entering(0)
        lax.fori_loop(0, levels, one, (start, jnp.zeros_like(start)), unroll=UNROLL)

    step(tracer, first, 0)
    edges[4] = wind_low * (2.0 * first[:, 0, :] + 5.0 * near - low[0]) * sixth
    step(first, second, 3)

    def to_rows(i, carry):
        off = pl.multiple_of(i * 128, 128)
        for s, ref in enumerate((first, second)):
            for h in range(2):
                block = ref[:, h * 8 : h * 8 + 8, pl.ds(off, 128)].reshape(128, 128)
                at = pl.multiple_of(s * SLOT_ROWS + h * width_y + off, 128)
                table[pl.ds(at, 128), :] = block.T
        return carry

    lax.fori_loop(0, width_y // 128, to_rows, 0)


def forward(*fields):
    vmem = pl.BlockSpec(memory_space=pltpu.VMEM)
    shape = fields[0].shape
    return pl.pallas_call(
        forward_kernel,
        out_shape=jax.ShapeDtypeStruct((2 * SLOT_ROWS, 128), jnp.float32),
        in_specs=[vmem] * len(fields),
        out_specs=vmem,
        scratch_shapes=[pltpu.VMEM(shape, jnp.float32)] * 2
        + [pltpu.VMEM((6, shape[0], shape[2]), jnp.float32)],
        compiler_params=pltpu.CompilerParams(vmem_limit_bytes=6 * 2**20),
    )(*fields)


def program(
    checkpoint,
    adjoint_in,
    courant_x,
    courant_y,
    mixing,
    snd_column,
    snd_count,
    snd_step,
    snd_value,
    snd_weight,
    snd_kernel,
):
    tiles = snd_column.shape[1]
    fields = (snd_count, snd_column, snd_step, snd_value, snd_weight, snd_kernel)
    fields += (courant_x, courant_y, mixing, adjoint_in)
    *fields, adjoint_in = (pltpu.with_memory_space_constraint(x, pltpu.HBM) for x in fields)
    winds = fields[6:]
    tracer = shifted(checkpoint, tiles)
    packed = pack(*fields[:6])
    box = lax.all_to_all(packed, "tile", split_axis=0, concat_axis=0, tiled=True)
    to_high, to_low, *near_winds = rims(tracer, *winds)
    low = shifted(to_high, 1)
    high = shifted(to_low, -1)
    table = forward(tracer, low, high, *near_winds)
    forcing_0, swept_1, to_low, to_high, *near_winds = adjoint_to_edges(
        table, box, adjoint_in, *winds
    )
    from_high = shifted(to_low, -1)
    from_low = shifted(to_high, 1)
    return adjoint_final(
        swept_1, forcing_0, *near_winds, from_low, from_high, low, high
    )


def solution(mesh):
    return jax.shard_map(
        program,
        mesh=mesh,
        in_specs=(P(None, RING, None),) * 5
        + (P(RING, None, None), P(RING, None))
        + (P(RING, None, None),) * 3
        + (P(RING, None, None, None),),
        out_specs=P(None, RING, None),
        check_vma=False,
    )
```

```python
import jax
import jax.numpy as jnp
from jax import lax
from jax.experimental import pallas as pl
from jax.experimental.pallas import tpu as pltpu
from jax.sharding import PartitionSpec as P


RING = ("group", "tile")
SLOT_ROWS = 1536
UNROLL = 4


def shifted(block, distance):
    total = lax.axis_size(RING)
    return lax.ppermute(block, RING, [(i, (i + distance) % total) for i in range(total)])


def flux_y(v, courant):
    width, axis = v.shape[-1], v.ndim - 1
    ahead, behind = pltpu.roll(v, width - 1, axis), pltpu.roll(v, 1, axis)
    f = courant * (2.0 * ahead + 5.0 * v - behind) * (1.0 / 6.0)
    return v + pltpu.roll(f, 1, axis) - f


def sweep_y(a, courant):
    width, axis = a.shape[-1], a.ndim - 1
    g = courant * (pltpu.roll(a, width - 1, axis) - a)
    return a + (2.0 * pltpu.roll(g, 1, axis) + 5.0 * g - pltpu.roll(g, width - 1, axis)) * (1.0 / 6.0)


def mix_rows(c, mixing):
    levels = c.shape[0]
    f = mixing * (pltpu.roll(c, levels - 1, 0) - c)
    return c + f - pltpu.roll(f, 1, 0)


def mixing_row(mixing, x):
    row = mixing[:, x, :]
    return jnp.concatenate([row, jnp.zeros((1, row.shape[1]), row.dtype)], axis=0)


def sounding_kernel(
    table,
    box,
    far_adjoint,
    far_courant_x,
    far_courant_y,
    far_mixing,
    forcing_0,
    forcing_1,
    to_low,
    to_high,
    courant_x,
    courant_y,
    mixing,
    adjoint_in,
    field_done,
    row_wide,
    row_ref,
    row_done,
    taken_0,
    taken_1,
    spread_0,
    spread_1,
    *sums,
):
    tiles = box.shape[0]
    width_y = adjoint_in.shape[2]

    def rows_of(t, carry):
        column = box[t, :, 17 * 128 : 18 * 128].astype(jnp.int32)
        step = box[t, :, 18 * 128 :].astype(jnp.int32)
        row = step * SLOT_ROWS + column // (8 * width_y) * width_y + column % width_y
        row_wide[pl.ds(t, 1), :] = row
        return carry

    lax.fori_loop(0, tiles, rows_of, 0, unroll=8)
    copy_rows = pltpu.make_async_copy(row_wide, row_ref, row_done)
    copy_rows.start()
    pairs = (
        (far_adjoint, adjoint_in),
        (far_courant_x, courant_x),
        (far_courant_y, courant_y),
        (far_mixing, mixing),
    )
    copies = [pltpu.make_async_copy(*pair, field_done.at[n]) for n, pair in enumerate(pairs)]
    for copy in copies:
        copy.start()

    def clear(i, carry):
        for acc in sums:
            acc[pl.ds(pl.multiple_of(i * 128, 128), 128), :] = jnp.zeros((128, 128), jnp.float32)
        return carry

    lax.fori_loop(0, 24, clear, 0)
    copy_rows.wait()

    sub = lax.broadcasted_iota(jnp.int32, (8, 128), 0)

    def gather(t, taken):
        for k in range(128):
            taken[k : k + 1, :] = table[pl.ds(row_ref[t, k], 1), :]

    def observe(t, taken, spread):
        cells = taken[...].T
        rows = [box[t, :, f * 128 : f * 128 + 128] for f in range(18)]
        total = cells[0:8, :] * rows[0]
        for level in range(1, 16):
            total = total + cells[level * 8 : level * 8 + 8, :] * rows[level]
        own = sub == (rows[17].astype(jnp.int32) // 768) % 8
        observed = jnp.sum(jnp.where(own, total, 0.0), axis=0, keepdims=True)
        misfit = jnp.where(own, jnp.broadcast_to(observed - rows[16], (8, 128)), 0.0)
        spread[...] = jnp.concatenate([misfit * rows[level] for level in range(16)], axis=0).T

    def scatter(t, spread):
        for k in range(128):
            acc = sums[k % len(sums)]
            at = pl.ds(row_ref[t, k], 1)
            acc[at, :] = acc[at, :] + spread[k : k + 1, :]

    spread_1[...] = jnp.zeros((128, 128), jnp.float32)
    gather(0, taken_0)

    def two(i, carry):
        t = 2 * i
        observe(t, taken_0, spread_0)
        gather(t + 1, taken_1)
        scatter(jnp.maximum(t - 1, 0), spread_1)
        observe(t + 1, taken_1, spread_1)
        gather(jnp.minimum(t + 2, tiles - 1), taken_0)
        scatter(t, spread_0)
        return carry

    lax.fori_loop(0, tiles // 2, two, 0)
    scatter(tiles - 1, spread_1)

    def back(i, carry):
        off = pl.multiple_of(i * 128, 128)
        for s, ref in enumerate((forcing_0, forcing_1)):
            for h in range(2):
                at = pl.ds(pl.multiple_of(s * SLOT_ROWS + h * 768 + off, 128), 128)
                block = sums[0][at, :]
                for acc in sums[1:]:
                    block = block + acc[at, :]
                ref[:, h * 8 : h * 8 + 8, pl.ds(off, 128)] = block.T.reshape(16, 8, 128)
        return carry

    lax.fori_loop(0, 6, back, 0)
    for copy in copies:
        copy.wait()
    b = {}
    for x in (0, 1, 2, 3, 14, 15):
        entering = adjoint_in[:, x, :] + forcing_1[:, x, :]
        b[x] = sweep_y(mix_rows(entering, mixing_row(mixing, x)), courant_y[:, x, :])
    g = {x: courant_x[:, x, :] * (b[x + 1] - b[x]) for x in (0, 1, 2, 14)}
    to_low[0] = b[0]
    to_low[1] = g[0]
    to_low[2] = b[0] + (5.0 * g[0] - g[1]) * (1.0 / 6.0) + forcing_0[:, 0, :]
    a = b[1] + (2.0 * g[0] + 5.0 * g[1] - g[2]) * (1.0 / 6.0) + forcing_0[:, 1, :]
    to_low[3] = sweep_y(mix_rows(a, mixing_row(mixing, 1)), courant_y[:, 1, :])
    to_high[0] = b[15]
    to_high[1] = b[15] + g[14] * (1.0 / 3.0) + forcing_0[:, 15, :]


def adjoint_to_edges(table, box, adjoint_in, *winds):
    vmem, hbm = (pl.BlockSpec(memory_space=space) for space in (pltpu.VMEM, pltpu.HBM))
    levels, _, width_y = adjoint_in.shape
    edges = tuple(jax.ShapeDtypeStruct((n, levels, width_y), jnp.float32) for n in (4, 2))
    return pl.pallas_call(
        sounding_kernel,
        out_shape=shapes_of(adjoint_in, adjoint_in) + edges + shapes_of(*winds, adjoint_in),
        in_specs=[vmem] * 2 + [hbm] * 4,
        out_specs=(vmem,) * 8,
        scratch_shapes=[
            pltpu.SemaphoreType.DMA((4,)),
            pltpu.VMEM((box.shape[0], 128), jnp.int32),
            pltpu.SMEM((box.shape[0], 128), jnp.int32),
            pltpu.SemaphoreType.DMA,
        ]
        + [pltpu.VMEM((128, 128), jnp.float32)] * 4
        + [pltpu.VMEM((2 * SLOT_ROWS, 128), jnp.float32)] * 8,
        compiler_params=pltpu.CompilerParams(vmem_limit_bytes=26 * 2**20),
    )(table, box, adjoint_in, *winds)


def inner_kernel(adjoint_in, forcing_1, courant_y, mixing, swept_1):
    levels = adjoint_in.shape[0]

    def first_step(level, carry):
        here, below = carry
        above = jnp.minimum(level + 1, levels - 1)
        upper = adjoint_in[above] + forcing_1[above]
        flux = mixing[jnp.minimum(level, levels - 2)] * (upper - here)
        flux = jnp.where(level < levels - 1, flux, 0.0)
        swept_1[level] = sweep_y(here + flux - below, courant_y[level])
        return upper, flux

    start = adjoint_in[0] + forcing_1[0]
    lax.fori_loop(0, levels, first_step, (start, jnp.zeros_like(start)), unroll=UNROLL)


def adjoint_inner(*fields):
    vmem = pl.BlockSpec(memory_space=pltpu.VMEM)
    return pl.pallas_call(
        inner_kernel,
        out_shape=jax.ShapeDtypeStruct(fields[0].shape, jnp.float32),
        in_specs=[vmem] * len(fields),
        out_specs=vmem,
        compiler_params=pltpu.CompilerParams(vmem_limit_bytes=4 * 2**20),
    )(*fields)


def final_kernel(
    swept_1, forcing_0, courant_x, courant_y, mixing, low, high, rim_low, rim_high, out, edges
):
    levels, width_x = swept_1.shape[:2]
    wind_low, wind_high = rim_low.at[4:7], rim_high.at[2:5]
    sixth = 1.0 / 6.0
    b_first, b_next, b_last = swept_1[:, 0, :], swept_1[:, 1, :], swept_1[:, width_x - 1, :]
    g_low = wind_low[0] * (b_first - low[0])
    g_first = courant_x[:, 0, :] * (b_next - b_first)
    g_last = courant_x[:, width_x - 1, :] * (high[0] - b_last)
    before = sweep_y(mix_rows(low[1] + (5.0 * g_low - g_first) * sixth, wind_low[2]), wind_low[1])
    after = sweep_y(mix_rows(high[2] + g_last * (1.0 / 3.0), wind_high[2]), wind_high[1])
    edges[0] = g_low
    edges[1] = before
    edges[2] = after
    edges[3] = wind_high[0] * (high[3] - after)
    sub = lax.broadcasted_iota(jnp.int32, swept_1.shape[1:], 0)

    def up(field, row):
        return jnp.where(sub == width_x - 1, row, pltpu.roll(field, width_x - 1, 0))

    def down(field, row):
        return jnp.where(sub == 0, row, pltpu.roll(field, 1, 0))

    def sweep_x(field, courant, after_last, g_before, g_after):
        g = courant * (up(field, after_last) - field)
        return field + (2.0 * down(g, g_before) + 5.0 * g - up(g, g_after)) * sixth

    def entering(level):
        at = pl.ds(level, 1)
        swept = sweep_x(
            swept_1[level], courant_x[level], high[0, at, :], edges[0, at, :], high[1, at, :]
        )
        return swept + forcing_0[level]

    def second_step(level, carry):
        here, below = carry
        at = pl.ds(level, 1)
        upper = entering(jnp.minimum(level + 1, levels - 1))
        flux = mixing[jnp.minimum(level, levels - 2)] * (upper - here)
        flux = jnp.where(level < levels - 1, flux, 0.0)
        b = sweep_y(here + flux - below, courant_y[level])
        c = courant_x[level]
        g_before = wind_low[0, at, :] * (b[0:1, :] - edges[1, at, :])
        out[level] = sweep_x(b, c, edges[2, at, :], g_before, edges[3, at, :])
        return upper, flux

    start = entering(0)
    lax.fori_loop(0, levels, second_step, (start, jnp.zeros_like(start)), unroll=UNROLL)


def adjoint_final(*fields):
    vmem = pl.BlockSpec(memory_space=pltpu.VMEM)
    shape = fields[0].shape
    return pl.pallas_call(
        final_kernel,
        out_shape=jax.ShapeDtypeStruct(shape, jnp.float32),
        in_specs=[vmem] * len(fields),
        out_specs=vmem,
        scratch_shapes=[pltpu.VMEM((4, shape[0], shape[2]), jnp.float32)],
        compiler_params=pltpu.CompilerParams(vmem_limit_bytes=4 * 2**20),
    )(*fields)


def pack_kernel(count, *refs):
    sources, packed, local, root, done = refs[:5], refs[5], refs[6:11], refs[11], refs[12]
    copies = [
        pltpu.make_async_copy(source, target, done.at[n])
        for n, (source, target) in enumerate(zip(sources, local))
    ]
    for copy in copies:
        copy.start()
    column, step, value, weight, kernel = local
    tiles, capacity = column.shape[1:]
    levels = kernel.shape[2]
    position = lax.broadcasted_iota(jnp.int32, (1, capacity), 1)
    for copy in copies:
        copy.wait()
    for t in range(tiles):
        root[t : t + 1, :] = jnp.where(position < count[0, t], weight[0, t : t + 1, :], 0.0)
    root[...] = jnp.sqrt(root[...])

    def one(t, carry):
        at = pl.ds(t, 1)
        scale = root[at, :]
        rows = kernel[0, t] * scale
        for level in range(levels):
            packed[t, :, level * capacity : (level + 1) * capacity] = rows[level : level + 1, :]
        rest = (
            value[0, at, :] * scale,
            column[0, at, :].astype(jnp.float32),
            step[0, at, :].astype(jnp.float32),
        )
        for f, part in enumerate(rest, levels):
            packed[t, :, f * capacity : (f + 1) * capacity] = part
        return carry

    lax.fori_loop(0, tiles, one, 0, unroll=4)


def pack(count, *fields):
    _, tiles, levels, capacity = fields[4].shape
    vmem, hbm = (pl.BlockSpec(memory_space=space) for space in (pltpu.VMEM, pltpu.HBM))
    return pl.pallas_call(
        pack_kernel,
        out_shape=jax.ShapeDtypeStruct((tiles, 1, (levels + 3) * capacity), jnp.float32),
        in_specs=[pl.BlockSpec(memory_space=pltpu.SMEM)] + [hbm] * len(fields),
        out_specs=vmem,
        scratch_shapes=[pltpu.VMEM(x.shape, x.dtype) for x in fields]
        + [
            pltpu.VMEM((tiles, capacity), jnp.float32),
            pltpu.SemaphoreType.DMA((len(fields),)),
        ],
        compiler_params=pltpu.CompilerParams(vmem_limit_bytes=4 * 2**20),
    )(count, *fields)


def rim_kernel(*refs):
    sources, (to_high, to_low), local, done = refs[:3], refs[4:6], refs[6:9], refs[9]
    tracer = refs[3]
    copies = [
        pltpu.make_async_copy(source, target, done.at[n])
        for n, (source, target) in enumerate(zip(sources, local))
    ]
    for copy in copies:
        copy.start()
    for copy in copies:
        copy.wait()
    courant_x, courant_y, mixing = local
    last = tracer.shape[1] - 1
    sixth = 1.0 / 6.0
    c = {x: tracer[:, x, :] for x in (0, 1, last - 3, last - 2, last - 1, last)}
    w = {x: courant_x[:, x, :] for x in (0, last - 2, last - 1, last)}

    def flux(x):
        return w[x] * (2.0 * c[x + 1] + 5.0 * c[x] - c[x - 1]) * sixth

    inner = flux(last - 1)
    swept = flux_y(c[last - 1] + flux(last - 2) - inner, courant_y[:, last - 1, :])
    to_high[0] = mix_rows(swept, mixing_row(mixing, last - 1))
    known = w[last] * (5.0 * c[last] - c[last - 1]) * sixth
    to_high[1] = c[last] + inner - known
    to_high[2] = known
    to_high[3] = c[last]
    to_low[0] = c[0]
    to_low[1] = c[0] - w[0] * (2.0 * c[1] + 5.0 * c[0]) * sixth
    for ref, first, x in ((to_high, 4, last), (to_low, 2, 0)):
        ref[first] = courant_x[:, x, :]
        ref[first + 1] = courant_y[:, x, :]
        ref[first + 2] = mixing_row(mixing, x)


def shapes_of(*fields):
    return tuple(jax.ShapeDtypeStruct(x.shape, x.dtype) for x in fields)


def rims(tracer, *winds):
    vmem = pl.BlockSpec(memory_space=pltpu.VMEM)
    levels, _, width_y = tracer.shape
    edges = tuple(jax.ShapeDtypeStruct((n, levels, width_y), jnp.float32) for n in (7, 5))
    return pl.pallas_call(
        rim_kernel,
        out_shape=edges + shapes_of(*winds),
        in_specs=[pl.BlockSpec(memory_space=pltpu.HBM)] * len(winds) + [vmem],
        out_specs=(vmem,) * 5,
        scratch_shapes=[pltpu.SemaphoreType.DMA((len(winds),))],
        compiler_params=pltpu.CompilerParams(vmem_limit_bytes=8 * 2**20),
    )(*winds, tracer)


def forward_kernel(tracer, low, high, courant_x, courant_y, mixing, table, first, second, edges):
    levels, width_x, width_y = tracer.shape
    sixth = 1.0 / 6.0
    last = width_x - 1
    sub = lax.broadcasted_iota(jnp.int32, tracer.shape[1:], 0)
    wind_low, wind_high = low[4], high[2]
    c_first, c_last = tracer[:, 0, :], tracer[:, last, :]
    reach = wind_low * c_first * (1.0 / 3.0)
    edges[0] = low[3]
    edges[1] = low[2] + reach
    edges[2] = high[0]
    near = mix_rows(flux_y(low[1] - reach, low[5]), low[6])
    flux_last = (
        courant_x[:, last, :] * (2.0 * high[0] + 5.0 * c_last - tracer[:, last - 1, :]) * sixth
    )
    after = flux_y(high[1] + wind_high * c_last * sixth + flux_last, high[3])
    edges[3] = near
    edges[5] = mix_rows(after, high[4])

    def step(source, target, e):
        def entering(level):
            at = pl.ds(level, 1)
            c, w = source[level], courant_x[level]
            ahead = jnp.where(sub == last, edges[e + 2, at, :], pltpu.roll(c, last, 0))
            behind = jnp.where(sub == 0, edges[e, at, :], pltpu.roll(c, 1, 0))
            f = w * (2.0 * ahead + 5.0 * c - behind) * sixth
            swept = c + jnp.where(sub == 0, edges[e + 1, at, :], pltpu.roll(f, 1, 0)) - f
            return flux_y(swept, courant_y[level])

        def one(level, carry):
            here, below = carry
            upper = entering(jnp.minimum(level + 1, levels - 1))
            flux = mixing[jnp.minimum(level, levels - 2)] * (upper - here)
            flux = jnp.where(level < levels - 1, flux, 0.0)
            target[level] = here + flux - below
            return upper, flux

        start = entering(0)
        lax.fori_loop(0, levels, one, (start, jnp.zeros_like(start)), unroll=UNROLL)

    step(tracer, first, 0)
    edges[4] = wind_low * (2.0 * first[:, 0, :] + 5.0 * near - low[0]) * sixth
    step(first, second, 3)

    def to_rows(i, carry):
        off = pl.multiple_of(i * 128, 128)
        for s, ref in enumerate((first, second)):
            for h in range(2):
                block = ref[:, h * 8 : h * 8 + 8, pl.ds(off, 128)].reshape(128, 128)
                at = pl.multiple_of(s * SLOT_ROWS + h * width_y + off, 128)
                table[pl.ds(at, 128), :] = block.T
        return carry

    lax.fori_loop(0, width_y // 128, to_rows, 0)


def forward(*fields):
    vmem = pl.BlockSpec(memory_space=pltpu.VMEM)
    shape = fields[0].shape
    return pl.pallas_call(
        forward_kernel,
        out_shape=jax.ShapeDtypeStruct((2 * SLOT_ROWS, 128), jnp.float32),
        in_specs=[vmem] * len(fields),
        out_specs=vmem,
        scratch_shapes=[pltpu.VMEM(shape, jnp.float32)] * 2
        + [pltpu.VMEM((6, shape[0], shape[2]), jnp.float32)],
        compiler_params=pltpu.CompilerParams(vmem_limit_bytes=6 * 2**20),
    )(*fields)


def program(
    checkpoint,
    adjoint_in,
    courant_x,
    courant_y,
    mixing,
    snd_column,
    snd_count,
    snd_step,
    snd_value,
    snd_weight,
    snd_kernel,
):
    tiles = snd_column.shape[1]
    fields = (snd_count, snd_column, snd_step, snd_value, snd_weight, snd_kernel)
    fields += (courant_x, courant_y, mixing, adjoint_in)
    *fields, adjoint_in = (pltpu.with_memory_space_constraint(x, pltpu.HBM) for x in fields)
    winds = fields[6:]
    tracer = shifted(checkpoint, tiles)
    packed = pack(*fields[:6])
    box = lax.all_to_all(packed, "tile", split_axis=0, concat_axis=0, tiled=True)
    to_high, to_low, *near_winds = rims(tracer, *winds)
    low = shifted(to_high, 1)
    high = shifted(to_low, -1)
    table = forward(tracer, low, high, *near_winds)
    forcing_0, forcing_1, to_low, to_high, *near_winds, near_adjoint = adjoint_to_edges(
        table, box, adjoint_in, *winds
    )
    from_high = shifted(to_low, -1)
    from_low = shifted(to_high, 1)
    swept_1 = adjoint_inner(near_adjoint, forcing_1, *near_winds[1:])
    return adjoint_final(
        swept_1, forcing_0, *near_winds, from_low, from_high, low, high
    )


def solution(mesh):
    return jax.shard_map(
        program,
        mesh=mesh,
        in_specs=(P(None, RING, None),) * 5
        + (P(RING, None, None), P(RING, None))
        + (P(RING, None, None),) * 3
        + (P(RING, None, None, None),),
        out_specs=P(None, RING, None),
        check_vma=False,
    )
```
